32 devices in a mesh: dom: 32 (over z, y, x, core).
Axes of the slice: x: 2, y: 2, z: 4, core: 2. Of those that a mesh axis runs over, the one named last changes fastest.
Arguments:
- concentration: float32 [1024, 128], P('dom'), may hold values from 0 to 1
- reaction_rate: float32 [1024, 128], P('dom'), may hold values from 0.5 to 4
- step_size: float32 [1], replicated, may hold values from 1 to 2
- block_values: float32 [1024, 5, 128, 128], P('dom'), may hold values from -40 to 48, as said below
- block_columns: int32 [1024, 5], P('dom'), may hold values from 0 to 95, as said below
- row_lengths: int32 [1024], P('dom'), may hold values from 2 to 5, as said below
- send_lists: int32 [32, 4, 16], P('dom'), may hold values from 0 to 31, as said below
Outputs:
- next_concentration: float32 [1024, 128], P('dom')
The draws below stay inside these ranges and needn't reach their ends.
Inputs may be any that keep to these rules, and one draw needn't show every extreme that they name: `send_lists`: for every partition and offset index q (offsets -2, -1, +1, +2), 16 distinct local block indices. `block_columns`: slot 0 of a block row is the row's own local block; live slots name a local block (below 32) or a ghost slot 32 + q * 16 + g of a block that the partition at offset index q sends; slot 1 of local block row q, for q = 0..3, is a ghost slot of offset index q; slots at or past the row's length repeat the row's own local block. `row_lengths`: some block row has all 5 slots live. `block_values`: slot 0 of every block row holds 8 times the identity plus a full random block; the other slots hold full random blocks.
All inputs are finite; a program needn't handle non-finite values.
Results may differ from the reference program's by a relative error of at most 0.00016.
Values sent between devices are 32-bit elements; how exact they have to be, the bound alone decides.
A program may use at most 64 MiB of HBM per device.

```python
import math
import jax
import jax.numpy as jnp
from jax import lax

BLK = 128
BDEV = 32
NNZB = 5
GMAX = 16
KRYLOV = 3
RESTARTS = 2
NDEV = 32
NB = 1024


def ghost_counts(key):
    first_key, second_key = jax.random.split(jax.random.fold_in(key, 11))
    counts = jax.random.randint(first_key, (NDEV, 4), max(GMAX // 4, 1), GMAX + 1)
    fullest = jax.random.randint(second_key, (4,), 0, NDEV)
    devices = jnp.arange(NDEV)[:, None]
    return jnp.where(devices == fullest[None, :], GMAX, counts).astype(jnp.int32)


def lengths_drawn(key):
    first_key, second_key = jax.random.split(jax.random.fold_in(key, 23))
    lengths = jax.random.randint(first_key, (NB,), 2, NNZB + 1)
    longest = jax.random.randint(second_key, (), 0, NB)
    return jnp.where(jnp.arange(NB) == longest, NNZB, lengths).astype(jnp.int32)


def draw_row_lengths(key, part):
    return lengths_drawn(key)


def draw_send_lists(key, part):
    scores = jax.random.randint(jax.random.fold_in(key, 37), (NDEV, 4, BDEV), 0, 1 << 20) * BDEV + jnp.arange(BDEV)
    ordering = jnp.argsort(scores, axis=-1)
    return ordering[:, :, :GMAX].astype(jnp.int32)


def draw_block_columns(key, part):
    counts = ghost_counts(key)
    lengths = lengths_drawn(key)
    subkeys = jax.random.split(jax.random.fold_in(key, 53), 4)
    row_ids = jnp.arange(NB)
    device = row_ids // BDEV
    local_row = row_ids % BDEV
    positions = jnp.arange(NNZB)[None, :]
    forced = (positions == 1) & (local_row[:, None] < 4)
    variety = jax.random.randint(subkeys[0], (NB, NNZB), 0, 2)
    variety = jnp.where(forced, 1, variety)
    owned = jax.random.randint(subkeys[1], (NB, NNZB), 0, BDEV)
    within = jax.random.randint(subkeys[2], (NB, NNZB), 0, 4)
    within = jnp.where(forced, jnp.broadcast_to((local_row % 4)[:, None], (NB, NNZB)), within)
    drawn_bits = jax.random.randint(subkeys[3], (NB, NNZB), 0, 1 << 20)
    offsets = jnp.array([-2, -1, 1, 2])
    sender = (device[:, None] - offsets[within]) % NDEV
    ghost_slot = drawn_bits % counts[sender, within]
    ghost = BDEV + within * GMAX + ghost_slot
    picked = jnp.where(variety == 1, ghost, owned)
    picked = jnp.where(positions == 0, local_row[:, None], picked)
    picked = jnp.where(positions < lengths[:, None], picked, local_row[:, None])
    return picked.astype(jnp.int32)


def draw_block_values(key, part):
    first_key = jax.random.fold_in(jax.random.fold_in(key, 71), 0)
    spread = 4.0 / math.sqrt(BLK * NNZB)
    shape = (NB, NNZB, BLK, BLK)
    entries = jax.random.normal(first_key, shape, jnp.float32)
    diagonal = (jnp.arange(NNZB) == 0).astype(jnp.float32)[None, :, None, None] * jnp.eye(BLK, dtype=jnp.float32)[None, None] * 8.0
    return (entries * spread + diagonal).astype(jnp.float32)


def block_scale(own_key, extent, shards, low, high):
    loudness = 1.0
    for dim, blocks in shards:
        draws = jax.random.uniform(jax.random.fold_in(jax.random.fold_in(own_key, 6), dim), (blocks,), jnp.float32, low / len(shards), high / len(shards))
        loudness = loudness * jnp.repeat(jnp.exp(draws), extent[dim] // blocks).reshape((-1,) + (1,) * (len(extent) - 1 - dim))
    return loudness


def setup_inputs(seed: int = 0) -> dict:
    key_of = jax.random.split(jax.random.key(seed), 8)
    return {
        "concentration": jnp.clip(1.0 * jax.random.uniform(key_of[0], (NB, BLK), jnp.float32) ** block_scale(key_of[0], (NB, BLK), ((0, 32),), -0.2, 0.2), 0.0, 1.0),
        "reaction_rate": jnp.clip(jnp.exp(math.log(4.0) - 2.0794415 * jax.random.uniform(key_of[1], (NB, BLK), jnp.float32) ** block_scale(key_of[1], (NB, BLK), ((0, 32),), -0.2, 0.2)), 0.5, 4.0),
        "step_size": jnp.clip(jax.random.uniform(key_of[2], (1,), jnp.float32, 1.0, 2.0), 1.0, 2.0),
        "block_values": draw_block_values(jax.random.fold_in(key_of[7], 71), 0),
        "block_columns": draw_block_columns(jax.random.fold_in(key_of[7], 71), 0),
        "row_lengths": draw_row_lengths(jax.random.fold_in(key_of[7], 71), 0),
        "send_lists": draw_send_lists(jax.random.fold_in(key_of[7], 71), 0),
    }


epsilon = 1e-06
OFFSETS = (-2, -1, 1, 2)

def column_map(block_columns, send_lists):
    device = (jnp.arange(NB, dtype=jnp.int32) // BDEV)[:, None]
    ghost_index = jnp.maximum(block_columns - BDEV, 0)
    neighbour = ghost_index // GMAX
    ghost_slot = ghost_index % GMAX
    offsets = jnp.array(OFFSETS, jnp.int32)
    sender = (device - offsets[neighbour]) % NDEV
    remote = send_lists[sender, neighbour, ghost_slot]
    owned = device * BDEV + block_columns
    return jnp.where(block_columns < BDEV, owned, sender * BDEV + remote).astype(jnp.int32)

def product(block_values, columns, active, field):
    gathered = field[columns] * active[:, :, None]
    return jnp.einsum('bsij,bsj->bi', block_values, gathered, precision=lax.Precision.HIGHEST)

def phi_column(hessenberg, substep):
    order = hessenberg.shape[0]
    augmented = jnp.zeros((order + 1, order + 1), jnp.float32)
    augmented = augmented.at[:order, :order].set(substep * hessenberg).at[0, order].set(1.0)
    reduced = augmented / 64.0
    identity = jnp.eye(order + 1, dtype=jnp.float32)
    series = identity
    for degree in range(12, 0, -1):
        series = identity + jnp.dot(reduced, series, precision=lax.Precision.HIGHEST) / degree
    for square_turn in range(6):
        series = jnp.dot(series, series, precision=lax.Precision.HIGHEST)
    return series[:order, order]

def krylov(start, apply):
    magnitude = jnp.sqrt(jnp.sum(start * start) + epsilon)
    vectors = jnp.zeros((KRYLOV,) + start.shape, jnp.float32).at[0].set(start / magnitude)
    hessenberg = jnp.zeros((KRYLOV, KRYLOV), jnp.float32)
    for column in range(KRYLOV):
        mapped = apply(vectors[column])
        projection = jnp.einsum('kbi,bi->k', vectors, mapped, precision=lax.Precision.HIGHEST)
        mapped = mapped - jnp.einsum('k,kbi->bi', projection, vectors, precision=lax.Precision.HIGHEST)
        hessenberg = hessenberg.at[:, column].set(projection)
        if column + 1 < KRYLOV:
            length = jnp.sqrt(jnp.sum(mapped * mapped) + epsilon)
            hessenberg = hessenberg.at[column + 1, column].set(length)
            vectors = vectors.at[column + 1].set(mapped / length)
    return (magnitude, vectors, hessenberg)

def reference(concentration, reaction_rate, step_size, block_values, block_columns, row_lengths, send_lists):
    columns = column_map(block_columns, send_lists)
    active = (jnp.arange(NNZB, dtype=jnp.int32)[None, :] < row_lengths[:, None]).astype(jnp.float32)
    slope = reaction_rate * (1.0 - 2.0 * concentration)

    def apply(field):
        return slope * field - product(block_values, columns, active, field)
    forcing = reaction_rate * concentration * (1.0 - concentration) - product(block_values, columns, active, concentration)
    substep = step_size[0] / RESTARTS
    increment = jnp.zeros_like(concentration)
    for restart in range(RESTARTS):
        start = forcing if restart == 0 else apply(increment) + forcing
        magnitude, vectors, hessenberg = krylov(start, apply)
        weights = phi_column(hessenberg, substep)
        increment = increment + substep * magnitude * jnp.einsum('k,kbi->bi', weights, vectors, precision=lax.Precision.HIGHEST)
    return concentration + increment
```

```python
import functools

import jax
import jax.numpy as jnp
from jax import lax
from jax.experimental import pallas as pl
from jax.experimental.pallas import tpu as pltpu
from jax.sharding import PartitionSpec as P

KRYLOV = 3
RESTARTS = 2
OFFSETS = (-2, -1, 1, 2)
SHIFT = 8.0
SCALE = 4.0
GROUP = 8
EXCHANGES = 7
epsilon = 1e-06


def total(terms):
    result = terms[0]
    for term in terms[1:]:
        result = result + term
    return result


def quadratic(left, gram, right):
    return total(
        [a * total([gram[i][j] * b for j, b in enumerate(right)]) for i, a in enumerate(left)]
    )


def mapped_coefficients(c):
    result = [-SHIFT * c[0]]
    for i in range(1, len(c)):
        result.append(SCALE * c[i - 1] - SHIFT * c[i])
    result.append(SCALE * c[-1])
    return result


def subtract(a, weight, b):
    return [x - weight * b[i] if i < len(b) else x for i, x in enumerate(a)]


def multiply(a, b):
    size = len(a)
    result = []
    for i in range(size):
        row = []
        for j in range(size):
            terms = [
                a[i][k] * b[k][j]
                for k in range(size)
                if a[i][k] is not None and b[k][j] is not None
            ]
            row.append(total(terms) if terms else None)
        result.append(row)
    return result


def plus_identity(a, weight):
    return [
        [x * weight + 1.0 if i == j else x * weight for j, x in enumerate(row)]
        for i, row in enumerate(a)
    ]


def phi_column(hessenberg, substep):
    size = len(hessenberg)
    x = [
        [None if h is None else substep * h * (1.0 / 64.0) for h in row] for row in hessenberg
    ]
    one = jnp.ones_like(substep)
    zero = jnp.zeros_like(substep)
    series = [[one if i == j else zero for j in range(size)] for i in range(size)]
    for degree in range(12, 1, -1):
        series = plus_identity(multiply(x, series), 1.0 / degree)
    column = [series[i][0] * (1.0 / 64.0) for i in range(size)]
    power = plus_identity(multiply(x, series), 1.0)
    for turn in range(6):
        column = [
            total([power[i][k] * column[k] for k in range(size)]) + column[i] for i in range(size)
        ]
        if turn < 5:
            power = multiply(power, power)
    return column


def restart_coefficients(gram, substep):
    magnitude = jnp.sqrt(gram[0][0] + epsilon)
    basis = [[1.0 / magnitude]]
    hessenberg = [[None] * KRYLOV for _ in range(KRYLOV)]
    for column in range(KRYLOV):
        mapped = mapped_coefficients(basis[column])
        residue = mapped
        for k in range(column + 1):
            projection = quadratic(basis[k], gram, mapped)
            hessenberg[k][column] = projection
            residue = subtract(residue, projection, basis[k])
        if column + 1 < KRYLOV:
            squared = jnp.maximum(quadratic(residue, gram, residue), 0.0)
            length = jnp.sqrt(squared + epsilon)
            hessenberg[column + 1][column] = length
            inverse = 1.0 / length
            basis.append([x * inverse for x in residue])
    weights = phi_column(hessenberg, substep)
    factor = substep * magnitude
    return [
        factor * total([weights[k] * basis[k][i] for k in range(i, KRYLOV)]) for i in range(KRYLOV)
    ]


def kernel(n, *refs):
    (step_ref, columns_ref, lengths_ref, lists_ref, c_ref, r_ref, a_ref, y) = refs[:8]
    scratch = list(refs[8:])
    a, local, mixed = scratch[:3]
    extended = scratch[3 : 3 + EXCHANGES]
    packets = scratch[3 + EXCHANGES : 3 + 2 * EXCHANGES]
    rest = scratch[3 + 2 * EXCHANGES :]
    sums, partial = rest[:RESTARTS], rest[RESTARTS : 2 * RESTARTS]
    load_sem, send_sem, recv_sem, sum_send, sum_recv = rest[2 * RESTARTS :]

    bdev, width = c_ref.shape
    slots = columns_ref.shape[1]
    gmax = lists_ref.shape[1]
    blank = bdev + len(OFFSETS) * gmax
    groups = bdev // GROUP
    me = lax.axis_index("dom")

    loads = []
    for g in range(groups):
        rows = pl.ds(g * GROUP, GROUP)
        copy = pltpu.make_async_copy(a_ref.at[rows], a.at[rows], load_sem.at[g])
        copy.start()
        loads.append(copy)

    barrier = pltpu.get_barrier_semaphore()

    def greet(d, carry):
        pl.semaphore_signal(
            barrier,
            inc=1,
            device_id=(lax.rem(me + d, n),),
            device_id_type=pl.DeviceIdType.MESH,
        )
        return carry

    lax.fori_loop(1, n, greet, 0)

    def copies(e):
        return [
            pltpu.make_async_remote_copy(
                src_ref=packets[e].at[q],
                dst_ref=extended[e].at[pl.ds(bdev + q * gmax, gmax)],
                send_sem=send_sem.at[e, q],
                recv_sem=recv_sem.at[e, q],
                device_id=(lax.rem(me + offset + n, n),),
                device_id_type=pl.DeviceIdType.MESH,
            )
            for q, offset in enumerate(OFFSETS)
        ]

    def pack(e, field):
        local[...] = field
        extended[e][0:bdev, :] = field
        extended[e][blank:, :] = jnp.zeros((8, width), jnp.float32)
        for q in range(len(OFFSETS)):
            for g in range(gmax):
                packets[e][q, g : g + 1, :] = local[pl.ds(lists_ref[q, g], 1), :]

    def send(e):
        for copy in copies(e):
            copy.start()

    def arrive(e):
        for copy in copies(e):
            copy.wait_recv()

    row_of = lax.broadcasted_iota(jnp.int32, (GROUP, 2 * width), 0)

    def group_product(source, g):
        result = None
        for i in range(GROUP):
            row = g * GROUP + i
            length = lengths_ref[row]
            acc = None
            for t in range(slots):
                index = columns_ref[row, t]
                if t > 0:
                    index = jnp.where(t < length, index, blank)
                term = a[row, t] * source[pl.ds(index, 1), :]
                acc = term if acc is None else acc + term
            high = acc.astype(jnp.bfloat16)
            low = (acc - high.astype(jnp.float32)).astype(jnp.bfloat16)
            both = jnp.concatenate([high, low], axis=1)
            pick = jnp.where(row_of == i, 1.0, 0.0).astype(jnp.bfloat16)
            part = lax.dot_general(
                pick, both, (((1,), (1,)), ((), ())), preferred_element_type=jnp.float32
            )
            result = part if result is None else result + part
        return result

    def operator(source, first=False):
        def body(g, carry):
            if first:
                rows = pl.ds(pl.multiple_of(g * GROUP, GROUP), GROUP)
                pltpu.make_async_copy(a_ref.at[rows], a.at[rows], load_sem.at[g]).wait()
            y[pl.ds(pl.multiple_of(g * GROUP, GROUP), GROUP), :] = group_product(source, g)
            return carry

        lax.fori_loop(0, groups, body, 0)
        return y[...]

    lane = lax.broadcasted_iota(jnp.int32, (1, width), 1)

    def dots(fields):
        rows = jnp.zeros((1, width), jnp.float32)
        index = 0
        for i in range(len(fields)):
            for j in range(i, len(fields)):
                folded = jnp.sum(fields[i] * fields[j], axis=0, keepdims=True)
                value = jnp.sum(folded, axis=1, keepdims=True)
                rows = jnp.where(lane == index, value, rows)
                index += 1
        return rows

    def send_sums(turn, row):
        partial[turn][...] = row
        sums[turn][me] = row

        def one(d, carry):
            pltpu.make_async_remote_copy(
                src_ref=partial[turn],
                dst_ref=sums[turn].at[me],
                send_sem=sum_send.at[turn],
                recv_sem=sum_recv.at[turn],
                device_id=(lax.rem(me + d, n),),
                device_id_type=pl.DeviceIdType.MESH,
            ).start()
            return carry

        lax.fori_loop(1, n, one, 0)

    def gather_sums(turn, count):
        others = sums[turn].at[pl.ds(0, n - 1)]
        pltpu.make_async_copy(others, others, sum_recv.at[turn]).wait()
        row = jnp.sum(sums[turn][...], axis=0)
        gram = [[None] * count for _ in range(count)]
        index = 0
        for i in range(count):
            for j in range(i, count):
                value = jnp.sum(jnp.where(lane == index, row, 0.0), axis=1, keepdims=True)
                gram[i][j] = gram[j][i] = jnp.broadcast_to(value, (8, width))
                index += 1
        return gram

    def combine(weights, fields):
        return total(
            [
                jnp.concatenate([w] * (f.shape[0] // 8), axis=0) * f
                for w, f in zip(weights, fields)
            ]
        )

    concentration = c_ref[...]
    rate = r_ref[...]
    shifted = (rate * (1.0 - 2.0 * concentration) + SHIFT) * (1.0 / SCALE)
    substep = jnp.full((8, width), step_ref[0] * (1.0 / RESTARTS), jnp.float32)

    def apply(source, field):
        return shifted * field - operator(source) * (1.0 / SCALE)

    pack(0, concentration)
    pl.semaphore_wait(barrier, n - 1)
    send(0)
    arrive(0)
    field = rate * concentration * (1.0 - concentration) - operator(extended[0], first=True)

    fields = [field]
    for j in range(KRYLOV):
        pack(1 + j, field)
        send(1 + j)
        arrive(1 + j)
        field = apply(extended[1 + j], field)
        fields.append(field)

    pack(KRYLOV + 1, field)
    send_sums(0, dots(fields))
    send(KRYLOV + 1)
    d = restart_coefficients(gather_sums(0, KRYLOV + 1), substep)
    s = mapped_coefficients(d)
    s[0] = s[0] + 1.0
    start = combine(s, fields)
    arrive(KRYLOV + 1)
    mixed[0:bdev, :] = start
    mixed[bdev:blank, :] = combine(
        s, [extended[1 + j][bdev:blank, :] for j in range(KRYLOV + 1)]
    )
    mixed[blank:, :] = jnp.zeros((8, width), jnp.float32)
    base = concentration + combine(d, fields[:KRYLOV])

    field = apply(mixed, start)
    fields = [start, field]
    for j in range(1, KRYLOV):
        e = KRYLOV + 1 + j
        pack(e, field)
        send(e)
        arrive(e)
        field = apply(extended[e], field)
        fields.append(field)
    send_sums(1, dots(fields))
    d = restart_coefficients(gather_sums(1, KRYLOV + 1), substep)
    y[...] = base + combine(d, fields[:KRYLOV])

    for e in range(EXCHANGES):
        for copy in copies(e):
            copy.wait_send()
    for turn in range(RESTARTS):
        others = sums[turn].at[pl.ds(0, n - 1)]
        pltpu.make_async_copy(others, others, sum_send.at[turn]).wait()


def solution(mesh):
    n = mesh.shape["dom"]

    def shards(c, r, step, values, columns, lengths, lists):
        bdev, width = c.shape
        slots = columns.shape[1]
        sides, gmax = lists.shape[1:]
        tall = bdev + sides * gmax + 8
        f32 = jnp.float32
        smem = pl.BlockSpec(memory_space=pltpu.SMEM)
        vmem = pl.BlockSpec(memory_space=pltpu.VMEM)
        return pl.pallas_call(
            functools.partial(kernel, n),
            out_shape=jax.ShapeDtypeStruct((bdev, width), f32),
            in_specs=[smem] * 4 + [vmem] * 2 + [pl.BlockSpec(memory_space=pl.ANY)],
            out_specs=vmem,
            scratch_shapes=[
                pltpu.VMEM((bdev, slots, width, width), f32),
                pltpu.VMEM((bdev, width), f32),
                pltpu.VMEM((tall, width), f32),
            ]
            + [pltpu.VMEM((tall, width), f32)] * EXCHANGES
            + [pltpu.VMEM((sides, gmax, width), f32)] * EXCHANGES
            + [pltpu.VMEM((n, 1, width), f32)] * RESTARTS
            + [pltpu.VMEM((1, width), f32)] * RESTARTS
            + [
                pltpu.SemaphoreType.DMA((bdev // GROUP,)),
                pltpu.SemaphoreType.DMA((EXCHANGES, sides)),
                pltpu.SemaphoreType.DMA((EXCHANGES, sides)),
                pltpu.SemaphoreType.DMA((RESTARTS,)),
                pltpu.SemaphoreType.DMA((RESTARTS,)),
            ],
            compiler_params=pltpu.CompilerParams(
                collective_id=0, has_side_effects=True, vmem_limit_bytes=40 * 2**20
            ),
        )(step, columns, lengths, lists[0], c, r, values)

    placed = (
        P("dom", None),
        P("dom", None),
        P(),
        P("dom", None, None, None),
        P("dom", None),
        P("dom"),
        P("dom", None, None),
    )
    return jax.shard_map(
        shards, mesh=mesh, in_specs=placed, out_specs=P("dom", None), check_vma=False
    )
```

```python
import functools

import jax
import jax.numpy as jnp
from jax import lax
from jax.experimental import pallas as pl
from jax.experimental.pallas import tpu as pltpu
from jax.sharding import PartitionSpec as P

KRYLOV = 3
RESTARTS = 2
OFFSETS = (-2, -1, 1, 2)
SHIFT = 8.0
SCALE = 4.0
GROUP = 8
EXCHANGES = 7
epsilon = 1e-06


def total(terms):
    result = terms[0]
    for term in terms[1:]:
        result = result + term
    return result


def quadratic(left, gram, right):
    return total(
        [a * total([gram[i][j] * b for j, b in enumerate(right)]) for i, a in enumerate(left)]
    )


def mapped_coefficients(c):
    result = [-SHIFT * c[0]]
    for i in range(1, len(c)):
        result.append(SCALE * c[i - 1] - SHIFT * c[i])
    result.append(SCALE * c[-1])
    return result


def subtract(a, weight, b):
    return [x - weight * b[i] if i < len(b) else x for i, x in enumerate(a)]


def multiply(a, b):
    size = len(a)
    result = []
    for i in range(size):
        row = []
        for j in range(size):
            terms = [
                a[i][k] * b[k][j]
                for k in range(size)
                if a[i][k] is not None and b[k][j] is not None
            ]
            row.append(total(terms) if terms else None)
        result.append(row)
    return result


def plus_identity(a, weight):
    return [
        [x * weight + 1.0 if i == j else x * weight for j, x in enumerate(row)]
        for i, row in enumerate(a)
    ]


def phi_column(hessenberg, substep):
    size = len(hessenberg)
    x = [
        [None if h is None else substep * h * (1.0 / 64.0) for h in row] for row in hessenberg
    ]
    one = jnp.ones_like(substep)
    zero = jnp.zeros_like(substep)
    series = [[one if i == j else zero for j in range(size)] for i in range(size)]
    for degree in range(12, 1, -1):
        series = plus_identity(multiply(x, series), 1.0 / degree)
    column = [series[i][0] * (1.0 / 64.0) for i in range(size)]
    power = plus_identity(multiply(x, series), 1.0)
    for turn in range(6):
        column = [
            total([power[i][k] * column[k] for k in range(size)]) + column[i] for i in range(size)
        ]
        if turn < 5:
            power = multiply(power, power)
    return column


def restart_coefficients(gram, substep):
    magnitude = jnp.sqrt(gram[0][0] + epsilon)
    basis = [[1.0 / magnitude]]
    hessenberg = [[None] * KRYLOV for _ in range(KRYLOV)]
    for column in range(KRYLOV):
        mapped = mapped_coefficients(basis[column])
        residue = mapped
        for k in range(column + 1):
            projection = quadratic(basis[k], gram, mapped)
            hessenberg[k][column] = projection
            residue = subtract(residue, projection, basis[k])
        if column + 1 < KRYLOV:
            squared = jnp.maximum(quadratic(residue, gram, residue), 0.0)
            length = jnp.sqrt(squared + epsilon)
            hessenberg[column + 1][column] = length
            inverse = 1.0 / length
            basis.append([x * inverse for x in residue])
    weights = phi_column(hessenberg, substep)
    factor = substep * magnitude
    return [
        factor * total([weights[k] * basis[k][i] for k in range(i, KRYLOV)]) for i in range(KRYLOV)
    ]


def kernel(n, *refs):
    operands, a_ref, y = refs[:6], refs[6], refs[7]
    staged = refs[8:14]
    step_ref, columns_ref, lengths_ref, lists_ref, c_ref, r_ref = staged
    scratch = list(refs[14:])
    stage_sem, table, a, local, mixed = scratch[:5]
    extended = scratch[5 : 5 + EXCHANGES]
    packets = scratch[5 + EXCHANGES : 5 + 2 * EXCHANGES]
    rest = scratch[5 + 2 * EXCHANGES :]
    sums, partial = rest[:RESTARTS], rest[RESTARTS : 2 * RESTARTS]
    load_sem, send_sem, recv_sem, sum_send, sum_recv = rest[2 * RESTARTS :]

    bdev, width = c_ref.shape
    slots = columns_ref.shape[0]
    gmax = lists_ref.shape[1]
    blank = bdev + len(OFFSETS) * gmax
    groups = bdev // GROUP
    me = lax.axis_index("dom")

    stages = [
        pltpu.make_async_copy(source, target, stage_sem.at[i])
        for i, (source, target) in enumerate(zip(operands, staged))
    ]
    for copy in stages:
        copy.start()
    loads = []
    for g in range(groups):
        rows = pl.ds(g * GROUP, GROUP)
        copy = pltpu.make_async_copy(a_ref.at[rows], a.at[rows], load_sem.at[g])
        copy.start()
        loads.append(copy)

    barrier = pltpu.get_barrier_semaphore()

    def greet(d, carry):
        pl.semaphore_signal(
            barrier,
            inc=1,
            device_id=(lax.rem(me + d, n),),
            device_id_type=pl.DeviceIdType.MESH,
        )
        return carry

    lax.fori_loop(1, n, greet, 0)
    for copy in stages:
        copy.wait()

    def copies(e):
        return [
            pltpu.make_async_remote_copy(
                src_ref=packets[e].at[q],
                dst_ref=extended[e].at[pl.ds(bdev + q * gmax, gmax)],
                send_sem=send_sem.at[e, q],
                recv_sem=recv_sem.at[e, q],
                device_id=(lax.rem(me + offset + n, n),),
                device_id_type=pl.DeviceIdType.MESH,
            )
            for q, offset in enumerate(OFFSETS)
        ]

    def pack(e, field):
        local[...] = field
        extended[e][0:bdev, :] = field
        extended[e][blank:, :] = jnp.zeros((8, width), jnp.float32)
        for q in range(len(OFFSETS)):
            for g in range(gmax):
                packets[e][q, g : g + 1, :] = local[pl.ds(lists_ref[q, g], 1), :]

    def send(e):
        for copy in copies(e):
            copy.start()

    def arrive(e):
        for copy in copies(e):
            copy.wait_recv()

    row_of = lax.broadcasted_iota(jnp.int32, (GROUP, 2 * width), 0)

    def group_product(source, g):
        result = None
        for i in range(GROUP):
            row = g * GROUP + i
            acc = None
            for t in range(slots):
                term = a[row, t] * source[pl.ds(table[row * slots + t], 1), :]
                acc = term if acc is None else acc + term
            high = acc.astype(jnp.bfloat16)
            low = (acc - high.astype(jnp.float32)).astype(jnp.bfloat16)
            both = jnp.concatenate([high, low], axis=1)
            pick = jnp.where(row_of == i, 1.0, 0.0).astype(jnp.bfloat16)
            part = lax.dot_general(
                pick, both, (((1,), (1,)), ((), ())), preferred_element_type=jnp.float32
            )
            result = part if result is None else result + part
        return result

    def operator(source, first=False):
        def body(g, carry):
            if first:
                rows = pl.ds(pl.multiple_of(g * GROUP, GROUP), GROUP)
                pltpu.make_async_copy(a_ref.at[rows], a.at[rows], load_sem.at[g]).wait()
            y[pl.ds(pl.multiple_of(g * GROUP, GROUP), GROUP), :] = group_product(source, g)
            return carry

        lax.fori_loop(0, groups, body, 0)
        return y[...]

    lane = lax.broadcasted_iota(jnp.int32, (1, width), 1)

    def dots(row, fields, last):
        for i in range(last + 1):
            folded = jnp.sum(fields[i] * fields[last], axis=0, keepdims=True)
            value = jnp.sum(folded, axis=1, keepdims=True)
            row = jnp.where(lane == last * (last + 1) // 2 + i, value, row)
        return row

    def send_sums(turn, row):
        partial[turn][...] = row
        sums[turn][me] = row

        def one(d, carry):
            pltpu.make_async_remote_copy(
                src_ref=partial[turn],
                dst_ref=sums[turn].at[me],
                send_sem=sum_send.at[turn],
                recv_sem=sum_recv.at[turn],
                device_id=(lax.rem(me + d, n),),
                device_id_type=pl.DeviceIdType.MESH,
            ).start()
            return carry

        lax.fori_loop(1, n, one, 0)

    def gather_sums(turn, count):
        others = sums[turn].at[pl.ds(0, n - 1)]
        pltpu.make_async_copy(others, others, sum_recv.at[turn]).wait()
        row = jnp.sum(sums[turn][...], axis=0)
        gram = [[None] * count for _ in range(count)]
        for j in range(count):
            for i in range(j + 1):
                index = j * (j + 1) // 2 + i
                value = jnp.sum(jnp.where(lane == index, row, 0.0), axis=1, keepdims=True)
                gram[i][j] = gram[j][i] = jnp.broadcast_to(value, (8, width))
        return gram

    def combine(weights, fields):
        return total(
            [
                jnp.concatenate([w] * (f.shape[0] // 8), axis=0) * f
                for w, f in zip(weights, fields)
            ]
        )

    concentration = c_ref[...]
    rate = r_ref[...]
    shifted = (rate * (1.0 - 2.0 * concentration) + SHIFT) * (1.0 / SCALE)
    substep = jnp.full((8, width), step_ref[0] * (1.0 / RESTARTS), jnp.float32)

    def apply(source, field):
        return shifted * field - operator(source) * (1.0 / SCALE)

    pack(0, concentration)
    pl.semaphore_wait(barrier, n - 1)
    send(0)

    def fill(row, carry):
        length = lengths_ref[row]
        for t in range(slots):
            table[row * slots + t] = jnp.where(t < length, columns_ref[t, row], blank)
        return carry

    lax.fori_loop(0, bdev, fill, 0)
    arrive(0)
    field = rate * concentration * (1.0 - concentration) - operator(extended[0], first=True)

    fields = [field]
    row = jnp.zeros((1, width), jnp.float32)
    for j in range(KRYLOV):
        pack(1 + j, field)
        send(1 + j)
        row = dots(row, fields, j)
        arrive(1 + j)
        field = apply(extended[1 + j], field)
        fields.append(field)

    e = KRYLOV + 1
    pack(e, field)
    send(e)
    send_sums(0, dots(row, fields, KRYLOV))
    arrive(e)
    field = apply(extended[e], field)
    fields.append(field)
    e = KRYLOV + 2
    pack(e, field)
    send(e)
    d = restart_coefficients(gather_sums(0, KRYLOV + 1), substep)
    s = mapped_coefficients(d)
    s[0] = s[0] + 1.0
    start = combine(s, fields[:-1])
    field = combine(s, fields[1:])
    base = concentration + combine(d, fields[:KRYLOV])
    mixed[0:bdev, :] = field
    mixed[blank:, :] = jnp.zeros((8, width), jnp.float32)
    fields = [start, field]
    row = jnp.zeros((1, width), jnp.float32)
    row = dots(dots(row, fields, 0), fields, 1)
    arrive(e)
    mixed[bdev:blank, :] = combine(
        s, [extended[2 + j][bdev:blank, :] for j in range(KRYLOV + 1)]
    )
    field = apply(mixed, field)
    fields.append(field)
    for j in range(2, KRYLOV):
        e = KRYLOV + 1 + j
        pack(e, field)
        send(e)
        row = dots(row, fields, j)
        arrive(e)
        field = apply(extended[e], field)
        fields.append(field)
    send_sums(1, dots(row, fields, KRYLOV))
    d = restart_coefficients(gather_sums(1, KRYLOV + 1), substep)
    y[...] = base + combine(d, fields[:KRYLOV])

    for e in range(EXCHANGES):
        for copy in copies(e):
            copy.wait_send()
    for turn in range(RESTARTS):
        others = sums[turn].at[pl.ds(0, n - 1)]
        pltpu.make_async_copy(others, others, sum_send.at[turn]).wait()


def solution(mesh):
    n = mesh.shape["dom"]

    def shards(c, r, step, values, columns, lengths, lists):
        bdev, width = c.shape
        slots = columns.shape[1]
        sides, gmax = lists.shape[1:]
        tall = bdev + sides * gmax + 8
        f32 = jnp.float32
        held = pl.BlockSpec(memory_space=pltpu.HBM)
        vmem = pl.BlockSpec(memory_space=pltpu.VMEM)
        return pl.pallas_call(
            functools.partial(kernel, n),
            out_shape=jax.ShapeDtypeStruct((bdev, width), f32),
            in_specs=[held] * 7,
            out_specs=vmem,
            scratch_shapes=[
                pltpu.SMEM((1,), f32),
                pltpu.SMEM((slots, bdev), jnp.int32),
                pltpu.SMEM((bdev,), jnp.int32),
                pltpu.SMEM((sides, gmax), jnp.int32),
                pltpu.VMEM((bdev, width), f32),
                pltpu.VMEM((bdev, width), f32),
                pltpu.SemaphoreType.DMA((6,)),
                pltpu.SMEM((bdev * slots,), jnp.int32),
                pltpu.VMEM((bdev, slots, width, width), f32),
                pltpu.VMEM((bdev, width), f32),
                pltpu.VMEM((tall, width), f32),
            ]
            + [pltpu.VMEM((tall, width), f32)] * EXCHANGES
            + [pltpu.VMEM((sides, gmax, width), f32)] * EXCHANGES
            + [pltpu.VMEM((n, 1, width), f32)] * RESTARTS
            + [pltpu.VMEM((1, width), f32)] * RESTARTS
            + [
                pltpu.SemaphoreType.DMA((bdev // GROUP,)),
                pltpu.SemaphoreType.DMA((EXCHANGES, sides)),
                pltpu.SemaphoreType.DMA((EXCHANGES, sides)),
                pltpu.SemaphoreType.DMA((RESTARTS,)),
                pltpu.SemaphoreType.DMA((RESTARTS,)),
            ],
            compiler_params=pltpu.CompilerParams(
                collective_id=0, has_side_effects=True, vmem_limit_bytes=67043328
            ),
        )(step, columns.T, lengths, lists[0], c, r, values)

    placed = (
        P("dom", None),
        P("dom", None),
        P(),
        P("dom", None, None, None),
        P("dom", None),
        P("dom"),
        P("dom", None, None),
    )
    return jax.shard_map(
        shards, mesh=mesh, in_specs=placed, out_specs=P("dom", None), check_vma=False
    )
```

```python
import functools

import jax
import jax.numpy as jnp
from jax import lax
from jax.experimental import pallas as pl
from jax.experimental.pallas import tpu as pltpu
from jax.sharding import PartitionSpec as P

KRYLOV = 3
RESTARTS = 2
OFFSETS = (-2, -1, 1, 2)
SHIFT = 8.0
SCALE = 4.0
GROUP = 8
EXCHANGES = 7
epsilon = 1e-06


def total(terms):
    result = terms[0]
    for term in terms[1:]:
        result = result + term
    return result


def quadratic(left, gram, right):
    return total(
        [a * total([gram[i][j] * b for j, b in enumerate(right)]) for i, a in enumerate(left)]
    )


def mapped_coefficients(c):
    result = [-SHIFT * c[0]]
    for i in range(1, len(c)):
        result.append(SCALE * c[i - 1] - SHIFT * c[i])
    result.append(SCALE * c[-1])
    return result


def subtract(a, weight, b):
    return [x - weight * b[i] if i < len(b) else x for i, x in enumerate(a)]


def multiply(a, b):
    size = len(a)
    result = []
    for i in range(size):
        row = []
        for j in range(size):
            terms = [
                a[i][k] * b[k][j]
                for k in range(size)
                if a[i][k] is not None and b[k][j] is not None
            ]
            row.append(total(terms) if terms else None)
        result.append(row)
    return result


def plus_identity(a, weight):
    return [
        [x * weight + 1.0 if i == j else x * weight for j, x in enumerate(row)]
        for i, row in enumerate(a)
    ]


def phi_column(hessenberg, substep):
    size = len(hessenberg)
    x = [
        [None if h is None else substep * h * (1.0 / 64.0) for h in row] for row in hessenberg
    ]
    one = jnp.ones_like(substep)
    zero = jnp.zeros_like(substep)
    series = [[one if i == j else zero for j in range(size)] for i in range(size)]
    for degree in range(12, 1, -1):
        series = plus_identity(multiply(x, series), 1.0 / degree)
    column = [series[i][0] * (1.0 / 64.0) for i in range(size)]
    power = plus_identity(multiply(x, series), 1.0)
    for turn in range(6):
        column = [
            total([power[i][k] * column[k] for k in range(size)]) + column[i] for i in range(size)
        ]
        if turn < 5:
            power = multiply(power, power)
    return column


def restart_coefficients(gram, substep):
    magnitude = jnp.sqrt(gram[0][0] + epsilon)
    basis = [[1.0 / magnitude]]
    hessenberg = [[None] * KRYLOV for _ in range(KRYLOV)]
    for column in range(KRYLOV):
        mapped = mapped_coefficients(basis[column])
        residue = mapped
        for k in range(column + 1):
            projection = quadratic(basis[k], gram, mapped)
            hessenberg[k][column] = projection
            residue = subtract(residue, projection, basis[k])
        if column + 1 < KRYLOV:
            squared = jnp.maximum(quadratic(residue, gram, residue), 0.0)
            length = jnp.sqrt(squared + epsilon)
            hessenberg[column + 1][column] = length
            inverse = 1.0 / length
            basis.append([x * inverse for x in residue])
    weights = phi_column(hessenberg, substep)
    factor = substep * magnitude
    return [
        factor * total([weights[k] * basis[k][i] for k in range(i, KRYLOV)]) for i in range(KRYLOV)
    ]


def kernel(n, *refs):
    operands, a_ref, y = refs[:6], refs[6], refs[7]
    staged = refs[8:14]
    step_ref, columns_ref, lengths_ref, lists_ref, c_ref, r_ref = staged
    scratch = list(refs[14:])
    stage_sem, table, a, local, mixed = scratch[:5]
    extended = scratch[5 : 5 + EXCHANGES]
    packets = scratch[5 + EXCHANGES : 5 + 2 * EXCHANGES]
    rest = scratch[5 + 2 * EXCHANGES :]
    sums, partial = rest[:RESTARTS], rest[RESTARTS : 2 * RESTARTS]
    load_sem, send_sem, recv_sem, sum_send, sum_recv = rest[2 * RESTARTS :]

    bdev, width = c_ref.shape
    slots = columns_ref.shape[0]
    gmax = lists_ref.shape[1]
    blank = bdev + len(OFFSETS) * gmax
    groups = bdev // GROUP
    me = lax.axis_index("dom")

    stages = [
        pltpu.make_async_copy(source, target, stage_sem.at[i])
        for i, (source, target) in enumerate(zip(operands, staged))
    ]
    for copy in stages:
        copy.start()
    loads = []
    for g in range(groups):
        rows = pl.ds(g * GROUP, GROUP)
        copy = pltpu.make_async_copy(a_ref.at[rows], a.at[rows], load_sem.at[g])
        copy.start()
        loads.append(copy)

    barrier = pltpu.get_barrier_semaphore()

    def greet(d, carry):
        pl.semaphore_signal(
            barrier,
            inc=1,
            device_id=(lax.rem(me + d, n),),
            device_id_type=pl.DeviceIdType.MESH,
        )
        return carry

    lax.fori_loop(1, n, greet, 0)
    for copy in stages:
        copy.wait()

    def copies(e):
        return [
            pltpu.make_async_remote_copy(
                src_ref=packets[e].at[q],
                dst_ref=extended[e].at[pl.ds(bdev + q * gmax, gmax)],
                send_sem=send_sem.at[e, q],
                recv_sem=recv_sem.at[e, q],
                device_id=(lax.rem(me + offset + n, n),),
                device_id_type=pl.DeviceIdType.MESH,
            )
            for q, offset in enumerate(OFFSETS)
        ]

    def pack(e, field):
        local[...] = field
        for q in range(len(OFFSETS)):
            for g in range(gmax):
                packets[e][q, g : g + 1, :] = local[pl.ds(lists_ref[q, g], 1), :]

    def send(e):
        for copy in copies(e):
            copy.start()
        extended[e][0:bdev, :] = local[...]
        extended[e][blank:, :] = jnp.zeros((8, width), jnp.float32)

    def arrive(e):
        for copy in copies(e):
            copy.wait_recv()

    row_of = lax.broadcasted_iota(jnp.int32, (GROUP, 2 * width), 0)

    def group_product(source, g):
        result = None
        for i in range(GROUP):
            row = g * GROUP + i
            acc = None
            for t in range(slots):
                term = a[row, t] * source[pl.ds(table[row * slots + t], 1), :]
                acc = term if acc is None else acc + term
            high = acc.astype(jnp.bfloat16)
            low = (acc - high.astype(jnp.float32)).astype(jnp.bfloat16)
            both = jnp.concatenate([high, low], axis=1)
            pick = jnp.where(row_of == i, 1.0, 0.0).astype(jnp.bfloat16)
            part = lax.dot_general(
                pick, both, (((1,), (1,)), ((), ())), preferred_element_type=jnp.float32
            )
            result = part if result is None else result + part
        return result

    def operator(source):
        return jnp.concatenate([group_product(source, g) for g in range(groups)], axis=0)

    lane = lax.broadcasted_iota(jnp.int32, (1, width), 1)

    def dots(row, fields, last):
        for i in range(last + 1):
            folded = jnp.sum(fields[i] * fields[last], axis=0, keepdims=True)
            value = jnp.sum(folded, axis=1, keepdims=True)
            row = jnp.where(lane == last * (last + 1) // 2 + i, value, row)
        return row

    def send_sums(turn, row):
        partial[turn][...] = row
        sums[turn][me] = row

        def one(d, carry):
            pltpu.make_async_remote_copy(
                src_ref=partial[turn],
                dst_ref=sums[turn].at[me],
                send_sem=sum_send.at[turn],
                recv_sem=sum_recv.at[turn],
                device_id=(lax.rem(me + d, n),),
                device_id_type=pl.DeviceIdType.MESH,
            ).start()
            return carry

        lax.fori_loop(1, n, one, 0)

    def gather_sums(turn, count):
        others = sums[turn].at[pl.ds(0, n - 1)]
        pltpu.make_async_copy(others, others, sum_recv.at[turn]).wait()
        row = jnp.sum(sums[turn][...], axis=0)
        gram = [[None] * count for _ in range(count)]
        for j in range(count):
            for i in range(j + 1):
                index = j * (j + 1) // 2 + i
                value = jnp.sum(jnp.where(lane == index, row, 0.0), axis=1, keepdims=True)
                gram[i][j] = gram[j][i] = jnp.broadcast_to(value, (8, width))
        return gram

    def combine(weights, fields):
        return total(
            [
                jnp.concatenate([w] * (f.shape[0] // 8), axis=0) * f
                for w, f in zip(weights, fields)
            ]
        )

    concentration = c_ref[...]
    rate = r_ref[...]
    shifted = (rate * (1.0 - 2.0 * concentration) + SHIFT) * (1.0 / SCALE)
    substep = jnp.full((8, width), step_ref[0] * (1.0 / RESTARTS), jnp.float32)

    def apply(source, field):
        return shifted * field - operator(source) * (1.0 / SCALE)

    pack(0, concentration)
    pl.semaphore_wait(barrier, n - 1)
    send(0)

    def fill(row, carry):
        length = lengths_ref[row]
        for t in range(slots):
            table[row * slots + t] = jnp.where(t < length, columns_ref[t, row], blank)
        return carry

    lax.fori_loop(0, bdev, fill, 0)
    for copy in loads:
        copy.wait()
    arrive(0)
    field = rate * concentration * (1.0 - concentration) - operator(extended[0])

    fields = [field]
    row = jnp.zeros((1, width), jnp.float32)
    for j in range(KRYLOV):
        pack(1 + j, field)
        send(1 + j)
        row = dots(row, fields, j)
        arrive(1 + j)
        field = apply(extended[1 + j], field)
        fields.append(field)

    e = KRYLOV + 1
    pack(e, field)
    send(e)
    send_sums(0, dots(row, fields, KRYLOV))
    arrive(e)
    field = apply(extended[e], field)
    fields.append(field)
    e = KRYLOV + 2
    pack(e, field)
    send(e)
    d = restart_coefficients(gather_sums(0, KRYLOV + 1), substep)
    s = mapped_coefficients(d)
    s[0] = s[0] + 1.0
    start = combine(s, fields[:-1])
    field = combine(s, fields[1:])
    base = concentration + combine(d, fields[:KRYLOV])
    mixed[0:bdev, :] = field
    mixed[blank:, :] = jnp.zeros((8, width), jnp.float32)
    fields = [start, field]
    row = jnp.zeros((1, width), jnp.float32)
    row = dots(dots(row, fields, 0), fields, 1)
    arrive(e)
    mixed[bdev:blank, :] = combine(
        s, [extended[2 + j][bdev:blank, :] for j in range(KRYLOV + 1)]
    )
    field = apply(mixed, field)
    fields.append(field)
    for j in range(2, KRYLOV):
        e = KRYLOV + 1 + j
        pack(e, field)
        send(e)
        row = dots(row, fields, j)
        arrive(e)
        field = apply(extended[e], field)
        fields.append(field)
    send_sums(1, dots(row, fields, KRYLOV))
    d = restart_coefficients(gather_sums(1, KRYLOV + 1), substep)
    y[...] = base + combine(d, fields[:KRYLOV])

    for e in range(EXCHANGES):
        for copy in copies(e):
            copy.wait_send()
    for turn in range(RESTARTS):
        others = sums[turn].at[pl.ds(0, n - 1)]
        pltpu.make_async_copy(others, others, sum_send.at[turn]).wait()


def solution(mesh):
    n = mesh.shape["dom"]

    def shards(c, r, step, values, columns, lengths, lists):
        bdev, width = c.shape
        slots = columns.shape[1]
        sides, gmax = lists.shape[1:]
        tall = bdev + sides * gmax + 8
        f32 = jnp.float32
        held = pl.BlockSpec(memory_space=pltpu.HBM)
        vmem = pl.BlockSpec(memory_space=pltpu.VMEM)
        return pl.pallas_call(
            functools.partial(kernel, n),
            out_shape=jax.ShapeDtypeStruct((bdev, width), f32),
            in_specs=[held] * 7,
            out_specs=vmem,
            scratch_shapes=[
                pltpu.SMEM((1,), f32),
                pltpu.SMEM((slots, bdev), jnp.int32),
                pltpu.SMEM((bdev,), jnp.int32),
                pltpu.SMEM((sides, gmax), jnp.int32),
                pltpu.VMEM((bdev, width), f32),
                pltpu.VMEM((bdev, width), f32),
                pltpu.SemaphoreType.DMA((6,)),
                pltpu.SMEM((bdev * slots,), jnp.int32),
                pltpu.VMEM((bdev, slots, width, width), f32),
                pltpu.VMEM((bdev, width), f32),
                pltpu.VMEM((tall, width), f32),
            ]
            + [pltpu.VMEM((tall, width), f32)] * EXCHANGES
            + [pltpu.VMEM((sides, gmax, width), f32)] * EXCHANGES
            + [pltpu.VMEM((n, 1, width), f32)] * RESTARTS
            + [pltpu.VMEM((1, width), f32)] * RESTARTS
            + [
                pltpu.SemaphoreType.DMA((bdev // GROUP,)),
                pltpu.SemaphoreType.DMA((EXCHANGES, sides)),
                pltpu.SemaphoreType.DMA((EXCHANGES, sides)),
                pltpu.SemaphoreType.DMA((RESTARTS,)),
                pltpu.SemaphoreType.DMA((RESTARTS,)),
            ],
            compiler_params=pltpu.CompilerParams(
                collective_id=0, has_side_effects=True, vmem_limit_bytes=67043328
            ),
        )(step, columns.T, lengths, lists[0], c, r, values)

    placed = (
        P("dom", None),
        P("dom", None),
        P(),
        P("dom", None, None, None),
        P("dom", None),
        P("dom"),
        P("dom", None, None),
    )
    return jax.shard_map(
        shards, mesh=mesh, in_specs=placed, out_specs=P("dom", None), check_vma=False
    )
```
